32 devices in a mesh: ma: 16 (over z, x, core), af: 2 (over y).
Axes of the slice: x: 2, y: 2, z: 4, core: 2. Of those that a mesh axis runs over, the one named last changes fastest.
Arguments:
- coeffs: bfloat16 [512, 128, 2049], P('ma', 'af'), parts along dimension 1, may hold values from -6 to 6
- legendre: bfloat16 [512, 256, 2049], P('ma'), may hold values from -0.1875 to 0.1875
- assign: int32 [512], P('ma'), may hold values from 0 to 511, each once
Outputs:
- fourier: float32 [512, 128, 1024], P('ma', 'af'), parts along dimension 1
The draws below stay inside these ranges and needn't reach their ends.
There are 2 independent parts, one for each index of `af`. The reference program is written for one: setup_inputs(seed, part) draws one part's arguments, and reference() takes and returns one part's arrays. A program takes and returns all parts, laid end to end along the dimension named above; an argument that names none is the same for every part. Nothing has to cross between parts.
Inputs may be any that keep to these rules, and one draw needn't show every extreme that they name: Slot s carries the wavenumbers assign[s] and 2047 - assign[s]; every pair appears once.
All inputs are finite; a program needn't handle non-finite values.
Results may differ from the reference program's by a relative error of at most 0.0003.
Values sent between devices are 32-bit elements; how exact they have to be, the bound alone decides.
A program may use at most 128 MiB of HBM per device.

```python
import jax
import jax.numpy as jnp
from jax import lax

TRUNC = 2047
PAIRS = 512
HLAT = 256
FIELDS = 32
KP = 2049
COLS = 64


def block_scale(key, extent, pieces, low, high):
    level, own = 1.0, jax.random.fold_in(key, 6)
    for dim, blocks in pieces:
        heights = jnp.exp(jax.random.uniform(jax.random.fold_in(own, dim), (blocks,), jnp.float32, low / len(pieces), high / len(pieces)))
        level = level * jnp.repeat(heights, extent[dim] // blocks).reshape([-1 if axis == dim else 1 for axis in range(len(extent))])
    return level


def centred(rng, shape, scale, most, shards=(), held_as=jnp.bfloat16):
    gain = block_scale(rng, shape, shards, -0.22, 0.18) if shards else 1.0
    entries = jax.random.normal(rng, shape, jnp.float32) * scale * gain
    return jnp.minimum(jnp.maximum(entries, -most), most).astype(held_as)


def setup_inputs(seed: int = 0, part: int = 0) -> dict:
    seeds = jax.random.split(jax.random.key(seed), 4)
    part_keys = jax.random.split(jax.random.fold_in(seeds[3], part), 4)
    coeffs = centred(part_keys[0], (PAIRS, COLS, KP), 1.0, 6.0, ((0, 16),))
    legendre = centred(seeds[1], (PAIRS, HLAT, KP), (KP // 2) ** -0.5, 0.1875, ((0, 16),))
    assign = jax.random.permutation(seeds[2], PAIRS).astype(jnp.int32)
    return {"coeffs": coeffs, "legendre": legendre, "assign": assign}


def slot_values(legendre_rows, coeff_rows, pair):
    entry = jnp.arange(KP, dtype=jnp.int32)
    first_len = (TRUNC + 1 - pair).astype(jnp.int32)
    second = entry >= first_len
    degree_gap = jnp.where(second, entry - first_len, entry)
    odd_gap = (degree_gap % 2) == 1
    group_masks = jnp.stack([
        jnp.logical_and(jnp.logical_not(second), jnp.logical_not(odd_gap)),
        jnp.logical_and(jnp.logical_not(second), odd_gap),
        jnp.logical_and(second, jnp.logical_not(odd_gap)),
        jnp.logical_and(second, odd_gap)], axis=0).astype(jnp.float32)
    masked = coeff_rows.astype(jnp.float32)[None, :, :] * group_masks[:, None, :]
    partial_value = jnp.einsum('hk,gck->hcg', legendre_rows.astype(jnp.float32), masked)
    north_rows = partial_value[:, :, 0::2] + partial_value[:, :, 1::2]
    south_rows = partial_value[:, :, 0::2] - partial_value[:, :, 1::2]
    return jnp.concatenate([north_rows, south_rows[::-1]], axis=0)


def reference(coeffs, legendre, assign):
    def one_slot(items):
        return slot_values(items[0], items[1], items[2])

    values = lax.map(one_slot, (legendre, coeffs, assign))
    values = jnp.transpose(values, (1, 2, 0, 3)).reshape(2 * HLAT, 2 * FIELDS, 2 * PAIRS)
    column = jnp.arange(2 * PAIRS, dtype=jnp.int32)
    owner_pair = assign[column // 2]
    column_place = jnp.where(column % 2 == 0, owner_pair, 2 * PAIRS - 1 - owner_pair).astype(jnp.int32)
    fourier = jnp.zeros((2 * HLAT, 2 * FIELDS, 2 * PAIRS), jnp.float32)
    return fourier.at[:, :, column_place].set(values)
```

```python
import functools

import jax
import jax.numpy as jnp
from jax import lax
from jax.experimental import pallas as pl
from jax.experimental.pallas import tpu as pltpu
from jax.sharding import PartitionSpec as P

MESH = pl.DeviceIdType.MESH
BUFFERS = 3
LOADS = 4
SPAN = 256
CHUNK_ROWS = 4
EARLY_PART = 2


def mask_groups(first_len, coeff_ref, out_ref):
    columns = coeff_ref.shape[0]
    width = out_ref.shape[1]
    pack = 16
    entry = lax.broadcasted_iota(jnp.int32, (pack, width), 1)
    first = entry < first_len
    odd_gap = (jnp.where(first, entry, entry - first_len) & 1) == 1
    sign = jnp.where(odd_gap, -1.0, 1.0)
    scales = [
        jnp.where(first, 1.0, 0.0),
        jnp.where(first, 0.0, 1.0),
        jnp.where(first, sign, 0.0),
        jnp.where(first, 0.0, sign),
    ]
    scales = [scale.astype(out_ref.dtype) for scale in scales]
    for low in range(0, columns, pack):
        values = coeff_ref[low:low + pack, :width]
        for index, scale in enumerate(scales):
            at = index * columns + low
            out_ref[at:at + pack, :] = values * scale


def last_entries(first_len, coeff_ref, row_of, start):
    columns, width = coeff_ref.shape
    total = 0.0
    for entry in range(start, width):
        first = entry < first_len
        gap = jnp.where(first, entry, entry - first_len)
        sign = jnp.where((gap & 1) == 1, -1.0, 1.0)
        outer = coeff_ref[:, entry:entry + 1].astype(jnp.float32) * row_of(entry - start)
        kinds = [jnp.where(first, 1.0, 0.0), jnp.where(first, 0.0, 1.0)]
        kinds += [kind * sign for kind in kinds]
        total += jnp.concatenate([outer * kind for kind in kinds], axis=0)
    return total


def synthesis_kernel(
    assign_ref, coeffs_ref, legendre_ref, out_ref,
    coeff_buf, legendre_buf, rest, rest_wide, wide, functions, groups, send, recv, pair_row, pair_rows, pair_columns, place, high_rows, low_rows,
    coeff_sem, span_sem, rest_sem, send_sem, recv_sem, *, devices, early, chunk,
):
    me = lax.axis_index("ma")
    half = devices // 2
    side = me // half
    slots, columns, width = coeffs_ref.shape
    lat_half = legendre_ref.shape[2]
    held = functions.shape[0]
    spans = width // SPAN
    turns = 1 + slots // held
    lanes = 2 * columns
    band = send.shape[1] // slots
    total = devices * slots
    chunks = band // chunk
    by_slot = (devices, slots, band, lanes)
    outgoing = send.reshape(by_slot)
    incoming = recv.reshape(by_slot)

    def coeff_load(slot):
        buf = lax.rem(slot, BUFFERS)
        return pltpu.make_async_copy(coeffs_ref.at[slot], coeff_buf.at[buf], coeff_sem.at[buf])

    def span_load(index):
        buf = lax.rem(index, LOADS)
        group = jnp.maximum(index // spans - 1, 0)
        rows = pl.ds(lax.rem(index, spans) * SPAN, SPAN)
        source = legendre_ref.at[rows, pl.ds(pl.multiple_of(group * held, held), held), :]
        return pltpu.make_async_copy(source, legendre_buf.at[buf], span_sem.at[buf])

    def unpack(turn, members):
        def span_step(span, carry):
            index = turn * spans + span
            span_load(index).wait()
            buf = lax.rem(index, LOADS)
            for low in range(0, lat_half, 128):
                block = legendre_buf[buf, :, :, low:low + 128].astype(jnp.float32)
                wide[low // 128] = block.reshape(SPAN * held, 128)

            @pl.when(index + LOADS < turns * spans)
            def _():
                span_load(index + LOADS).start()

            at = pl.ds(pl.multiple_of(span * SPAN, SPAN), SPAN)
            for member in members:
                for low in range(0, lat_half, 128):
                    rows = wide[low // 128, pl.ds(member, SPAN, stride=held), :]
                    functions[member, at, low:low + 128] = rows.astype(functions.dtype)
            return carry

        lax.fori_loop(0, spans, span_step, 0)

    def for_peers(act):
        def across(k, carry):
            act((1 - side) * half + lax.rem(me + k, half))
            return carry

        def within(k, carry):
            act(side * half + lax.rem(me + k, half))
            return carry

        lax.fori_loop(0, half, across, 0)
        lax.fori_loop(1, half, within, 0)

    def copy(source, target, group, peer):
        return pltpu.make_async_remote_copy(
            src_ref=source,
            dst_ref=target,
            send_sem=send_sem.at[group],
            recv_sem=recv_sem.at[group],
            device_id={"ma": peer},
            device_id_type=MESH,
        )

    def compute(slot, member):
        coeff_load(slot).wait()
        buf = lax.rem(slot, BUFFERS)
        pair = assign_ref[slot]
        lane = lax.broadcasted_iota(jnp.int32, pair_row.shape, 1)
        pair_row[...] = jnp.where(lane == slot, pair, pair_row[...])
        first_len = width - 1 - pair
        mask_groups(first_len, coeff_buf.at[buf], groups)
        value = jnp.dot(groups[...], functions[member], preferred_element_type=jnp.float32)
        value += last_entries(first_len, coeff_buf.at[buf], lambda n: rest_wide[n, pl.ds(slot, 1), :], spans * SPAN)
        value = value.T
        at = pl.ds(pl.multiple_of(slot * band, band), band)
        for block in range(half):
            rows = slice(block * band, (block + 1) * band)
            send[block, at, :] = value[rows, :lanes]
            send[devices - 1 - block, at, :] = value[rows, lanes:]
        recv[me, at, :] = send[me, at, :]

        @pl.when(slot + BUFFERS < slots)
        def _():
            coeff_load(slot + BUFFERS).start()

    def send_slot(slot):
        for_peers(lambda peer: copy(outgoing.at[peer, slot], incoming.at[me, slot], 0, peer).start())

    def late(ref, device, first_row):
        return ref.at[device, pl.ds(early, slots - early), pl.ds(first_row, chunk), :]

    def send_chunk(index):
        row = index * chunk
        for_peers(lambda peer: copy(late(outgoing, peer, row), late(incoming, me, row), 1 + index, peer).start())

    for index in range(min(LOADS, turns * spans)):
        span_load(index).start()
    rest_load = pltpu.make_async_copy(legendre_ref.at[pl.ds(spans * SPAN, width - spans * SPAN)], rest, rest_sem)
    rest_load.start()
    for slot in range(min(BUFFERS, slots)):
        coeff_load(slot).start()
    barrier = pltpu.get_barrier_semaphore()
    for_peers(lambda peer: pl.semaphore_signal(barrier, inc=1, device_id={"ma": peer}, device_id_type=MESH))
    pair_row[...] = jnp.zeros_like(pair_row)
    rest_load.wait()
    rest_wide[...] = rest[...].astype(jnp.float32)
    unpack(0, [0])
    compute(0, 0)
    pl.semaphore_wait(barrier, devices - 1)
    send_slot(0)
    unpack(1, range(1, held))

    def member_step(group):
        def step(member, carry):
            slot = group * held + member
            compute(slot, member)

            @pl.when(slot < early)
            def _():
                send_slot(slot)

            return carry

        return step

    lax.fori_loop(1, held, member_step(0), 0)

    def group_step(group, carry):
        unpack(group + 1, range(held))
        lax.fori_loop(0, held, member_step(group), 0)
        return carry

    lax.fori_loop(1, slots // held, group_step, 0)

    pairs_group = 1 + chunks
    for_peers(lambda peer: copy(pair_row, pair_rows.at[me], pairs_group, peer).start())
    pair_rows[me] = pair_row[...]

    def chunk_step(index, carry):
        send_chunk(index)
        return carry

    lax.fori_loop(0, chunks, chunk_step, 0)

    others = pl.ds(0, devices - 1)
    whole = lambda ref: ref.at[others, pl.ds(0, early)]
    part = lambda ref, index: ref.at[others, pl.ds(early, slots - early), pl.ds(index * chunk, chunk), :]

    def wait_bytes(ref, sem):
        pltpu.make_async_copy(ref, ref, sem).wait()

    wait_bytes(pair_rows.at[others], recv_sem.at[pairs_group])

    def column_step(device, carry):
        row = pair_rows[device].astype(jnp.float32)
        rows = jnp.broadcast_to(row, (slots, row.shape[-1]))
        own = lax.broadcasted_iota(jnp.int32, rows.shape, 0) == lax.broadcasted_iota(jnp.int32, rows.shape, 1)
        column = jnp.sum(jnp.where(own, rows, 0.0), axis=1, keepdims=True)
        at = pl.ds(pl.multiple_of(device * slots, slots), slots)
        pair_columns[at, :] = jnp.broadcast_to(column, (slots, pair_columns.shape[1]))
        return carry

    lax.fori_loop(0, devices, column_step, 0)
    step = 64
    lane = lax.broadcasted_iota(jnp.int32, (step, total), 1)
    for low in range(0, total, step):
        pairs = pair_columns[low:low + step, :1].astype(jnp.int32)
        place[0, low:low + step, :] = (pairs == lane).astype(jnp.float32).astype(jnp.bfloat16)
        place[1, low:low + step, :] = (total - 1 - pairs == lane).astype(jnp.float32).astype(jnp.bfloat16)

    wait_bytes(whole(incoming), recv_sem.at[0])
    flat = recv.reshape(devices * slots * band, lanes)

    def place_step(index, carry):
        wait_bytes(part(incoming, index), recv_sem.at[1 + index])
        for i in range(chunk):
            row = index * chunk + i
            values = flat[pl.ds(row, total, stride=band), :].T
            high = values.astype(jnp.bfloat16)
            low = (values - high.astype(jnp.float32)).astype(jnp.bfloat16)
            for w in range(2):
                at = slice(i * columns, (i + 1) * columns)
                high_rows[w, at, :] = high[w * columns:(w + 1) * columns]
                low_rows[w, at, :] = low[w * columns:(w + 1) * columns]
        for w in range(2):
            placed = jnp.dot(high_rows[w], place[w], preferred_element_type=jnp.float32)
            placed += jnp.dot(low_rows[w], place[w], preferred_element_type=jnp.float32)
            for i in range(chunk):
                row = index * chunk + i
                to = row + side * (band - 1 - 2 * row)
                out_ref[to, :, w * total:(w + 1) * total] = placed[i * columns:(i + 1) * columns]
        return carry

    lax.fori_loop(0, chunks, place_step, 0)

    wait_bytes(whole(outgoing), send_sem.at[0])

    def drain_step(index, carry):
        wait_bytes(part(outgoing, index), send_sem.at[1 + index])
        return carry

    lax.fori_loop(0, chunks, drain_step, 0)
    wait_bytes(pair_rows.at[others], send_sem.at[pairs_group])


def shards(coeffs, legendre, assign):
    devices = lax.axis_size("ma")
    slots, columns, width = coeffs.shape
    lat_half = legendre.shape[1]
    band = 2 * lat_half // devices
    total = devices * slots
    lanes = 2 * columns
    chunk = min(CHUNK_ROWS, band)
    early = max(slots // EARLY_PART, 1)
    groups = 2 + band // chunk
    held = min(8, slots)
    main = width // SPAN * SPAN
    return pl.pallas_call(
        functools.partial(synthesis_kernel, devices=devices, early=early, chunk=chunk),
        out_shape=jax.ShapeDtypeStruct((band, columns, 2 * total), jnp.float32),
        in_specs=[
            pl.BlockSpec(memory_space=pltpu.SMEM),
            pl.BlockSpec(memory_space=pl.ANY),
            pl.BlockSpec(memory_space=pl.ANY),
        ],
        out_specs=pl.BlockSpec(memory_space=pltpu.VMEM),
        scratch_shapes=[
            pltpu.VMEM((BUFFERS, columns, width), jnp.bfloat16),
            pltpu.VMEM((LOADS, SPAN, held, lat_half), jnp.bfloat16),
            pltpu.VMEM((width - main, slots, lat_half), jnp.bfloat16),
            pltpu.VMEM((width - main, slots, lat_half), jnp.float32),
            pltpu.VMEM((lat_half // 128, SPAN * held, 128), jnp.float32),
            pltpu.VMEM((held, main, lat_half), jnp.bfloat16),
            pltpu.VMEM((4 * columns, main), jnp.bfloat16),
            pltpu.VMEM((devices, slots * band, lanes), jnp.float32),
            pltpu.VMEM((devices, slots * band, lanes), jnp.float32),
            pltpu.VMEM((1, lanes), jnp.int32),
            pltpu.VMEM((devices, 1, lanes), jnp.int32),
            pltpu.VMEM((total, lanes), jnp.float32),
            pltpu.VMEM((2, total, total), jnp.bfloat16),
            pltpu.VMEM((2, chunk * columns, total), jnp.bfloat16),
            pltpu.VMEM((2, chunk * columns, total), jnp.bfloat16),
            pltpu.SemaphoreType.DMA((BUFFERS,)),
            pltpu.SemaphoreType.DMA((LOADS,)),
            pltpu.SemaphoreType.DMA,
            pltpu.SemaphoreType.DMA((groups,)),
            pltpu.SemaphoreType.DMA((groups,)),
        ],
        compiler_params=pltpu.CompilerParams(
            collective_id=0, has_side_effects=True, vmem_limit_bytes=56 * 1024 * 1024
        ),
        name="synthesis",
    )(assign, coeffs, legendre.transpose(2, 0, 1))


def solution(mesh):
    return jax.shard_map(
        shards,
        mesh=mesh,
        in_specs=(P("ma", "af", None), P("ma", None, None), P("ma")),
        out_specs=P("ma", "af", None),
        check_vma=False,
    )
```

```python
import functools

import jax
import jax.numpy as jnp
from jax import lax
from jax.experimental import pallas as pl
from jax.experimental.pallas import tpu as pltpu
from jax.sharding import PartitionSpec as P

MESH = pl.DeviceIdType.MESH
BUFFERS = 3
LOADS = 8
NARROW = 2
SPAN = 256
CHUNK_ROWS = 2
EARLY_PART = 2


def mask_groups(first_len, coeff_ref, out_ref):
    columns = coeff_ref.shape[0]
    width = out_ref.shape[1]
    pack = 16
    entry = lax.broadcasted_iota(jnp.int32, (pack, width), 1)
    first = entry < first_len
    odd_gap = (jnp.where(first, entry, entry - first_len) & 1) == 1
    sign = jnp.where(odd_gap, -1.0, 1.0)
    scales = [
        jnp.where(first, 1.0, 0.0),
        jnp.where(first, 0.0, 1.0),
        jnp.where(first, sign, 0.0),
        jnp.where(first, 0.0, sign),
    ]
    scales = [scale.astype(out_ref.dtype) for scale in scales]
    for low in range(0, columns, pack):
        values = coeff_ref[low:low + pack, :width]
        for index, scale in enumerate(scales):
            at = index * columns + low
            out_ref[at:at + pack, :] = values * scale


def last_entries(first_len, coeff_ref, row_of, start):
    columns, width = coeff_ref.shape
    total = 0.0
    for entry in range(start, width):
        first = entry < first_len
        gap = jnp.where(first, entry, entry - first_len)
        sign = jnp.where((gap & 1) == 1, -1.0, 1.0)
        outer = coeff_ref[:, entry:entry + 1].astype(jnp.float32) * row_of(entry - start)
        kinds = [jnp.where(first, 1.0, 0.0), jnp.where(first, 0.0, 1.0)]
        kinds += [kind * sign for kind in kinds]
        total += jnp.concatenate([outer * kind for kind in kinds], axis=0)
    return total


def synthesis_kernel(
    assign_ref, coeffs_ref, legendre_ref, out_ref,
    coeff_buf, legendre_buf, rest, rest_wide, wide, functions, groups, send, recv, pair_row, pair_rows, pair_columns, place, high_rows, low_rows,
    coeff_sem, span_sem, rest_sem, send_sem, recv_sem, *, devices, early, chunk,
):
    me = lax.axis_index("ma")
    half = devices // 2
    side = me // half
    slots, columns, width = coeffs_ref.shape
    lat_half = legendre_ref.shape[2]
    held = functions.shape[0]
    spans = width // SPAN
    turns = 1 + slots // held
    parts = held // NARROW
    share = SPAN // parts
    lanes = 2 * columns
    band = send.shape[1] // slots
    total = devices * slots
    chunks = band // chunk
    by_slot = (devices, slots, band, lanes)
    outgoing = send.reshape(by_slot)
    incoming = recv.reshape(by_slot)

    def coeff_load(slot):
        buf = lax.rem(slot, BUFFERS)
        return pltpu.make_async_copy(coeffs_ref.at[slot], coeff_buf.at[buf], coeff_sem.at[buf])

    def span_load(index):
        buf = lax.rem(index, LOADS)
        rows = pl.ds(lax.rem(index, spans) * SPAN, SPAN)
        group = jnp.maximum(index // spans - 1, 0)
        source = legendre_ref.at[rows, pl.ds(pl.multiple_of(group * held, held), held), :]
        return pltpu.make_async_copy(source, legendre_buf.at[buf], span_sem.at[buf])

    def narrow_loads(span):
        buf = lax.rem(span, LOADS)
        return [
            pltpu.make_async_copy(
                legendre_ref.at[pl.ds(span * SPAN + part * share, share), pl.ds(0, NARROW), :],
                legendre_buf.at[buf, pl.ds(0, share), pl.ds(part * NARROW, NARROW), :],
                span_sem.at[buf],
            )
            for part in range(parts)
        ]

    def widen(buf, rows):
        for low in range(0, lat_half, 128):
            block = legendre_buf[buf, :rows, :, low:low + 128].astype(jnp.float32)
            wide[low // 128, :rows * held] = block.reshape(rows * held, 128)

    def pick(member, at, first, rows):
        for low in range(0, lat_half, 128):
            block = wide[low // 128, pl.ds(first, rows, stride=held), :]
            functions[member, at, low:low + 128] = block.astype(functions.dtype)

    def unpack_narrow():
        def span_step(span, carry):
            buf = lax.rem(span, LOADS)
            landed = legendre_buf.at[buf, pl.ds(0, share)]
            pltpu.make_async_copy(landed, landed, span_sem.at[buf]).wait()
            widen(buf, share)
            later = span + LOADS

            @pl.when(later < spans)
            def _():
                for load in narrow_loads(later):
                    load.start()

            @pl.when(later >= spans)
            def _():
                span_load(later).start()

            for member in range(NARROW):
                for part in range(parts):
                    at = pl.ds(pl.multiple_of(span * SPAN + part * share, share), share)
                    pick(member, at, part * NARROW + member, share)
            return carry

        lax.fori_loop(0, spans, span_step, 0)

    def unpack(turn, members):
        def span_step(span, carry):
            index = turn * spans + span
            span_load(index).wait()
            buf = lax.rem(index, LOADS)
            widen(buf, SPAN)

            @pl.when(index + LOADS < turns * spans)
            def _():
                span_load(index + LOADS).start()

            at = pl.ds(pl.multiple_of(span * SPAN, SPAN), SPAN)
            for member in members:
                pick(member, at, member, SPAN)
            return carry

        lax.fori_loop(0, spans, span_step, 0)

    def for_peers(act):
        def across(k, carry):
            act((1 - side) * half + lax.rem(me + k, half))
            return carry

        def within(k, carry):
            act(side * half + lax.rem(me + k, half))
            return carry

        lax.fori_loop(0, half, across, 0)
        lax.fori_loop(1, half, within, 0)

    def copy(source, target, group, peer):
        return pltpu.make_async_remote_copy(
            src_ref=source,
            dst_ref=target,
            send_sem=send_sem.at[group],
            recv_sem=recv_sem.at[group],
            device_id={"ma": peer},
            device_id_type=MESH,
        )

    def prepare(slot):
        coeff_load(slot).wait()
        buf = lax.rem(slot, BUFFERS)
        pair = assign_ref[slot]
        lane = lax.broadcasted_iota(jnp.int32, pair_row.shape, 1)
        pair_row[...] = jnp.where(lane == slot, pair, pair_row[...])
        first_len = width - 1 - pair
        mask_groups(first_len, coeff_buf.at[buf], groups)

    def compute(slot, member):
        buf = lax.rem(slot, BUFFERS)
        first_len = width - 1 - assign_ref[slot]
        value = jnp.dot(groups[...], functions[member], preferred_element_type=jnp.float32)
        value += last_entries(first_len, coeff_buf.at[buf], lambda n: rest_wide[n, pl.ds(slot, 1), :], spans * SPAN)
        value = value.T
        at = pl.ds(pl.multiple_of(slot * band, band), band)
        for block in range(half):
            rows = slice(block * band, (block + 1) * band)
            send[block, at, :] = value[rows, :lanes]
            send[devices - 1 - block, at, :] = value[rows, lanes:]
        recv[me, at, :] = send[me, at, :]

        @pl.when(slot + BUFFERS < slots)
        def _():
            coeff_load(slot + BUFFERS).start()

    def send_slot(slot):
        for_peers(lambda peer: copy(outgoing.at[peer, slot], incoming.at[me, slot], 0, peer).start())

    def late(ref, device, first_row):
        return ref.at[device, pl.ds(early, slots - early), pl.ds(first_row, chunk), :]

    def send_chunk(index):
        row = index * chunk
        for_peers(lambda peer: copy(late(outgoing, peer, row), late(incoming, me, row), 1 + index, peer).start())

    coeff_load(0).start()
    for index in range(min(LOADS, spans)):
        for load in narrow_loads(index):
            load.start()
    for index in range(spans, LOADS):
        span_load(index).start()
    rest_load = pltpu.make_async_copy(legendre_ref.at[pl.ds(spans * SPAN, width - spans * SPAN)], rest, rest_sem)
    rest_load.start()
    for slot in range(1, min(BUFFERS, slots)):
        coeff_load(slot).start()
    barrier = pltpu.get_barrier_semaphore()
    for_peers(lambda peer: pl.semaphore_signal(barrier, inc=1, device_id={"ma": peer}, device_id_type=MESH))
    pair_row[...] = jnp.zeros_like(pair_row)
    prepare(0)
    rest_load.wait()
    rest_wide[...] = rest[...].astype(jnp.float32)
    unpack_narrow()
    compute(0, 0)
    pl.semaphore_wait(barrier, devices - 1)
    send_slot(0)
    for slot in range(1, NARROW):
        prepare(slot)
        compute(slot, slot)
        send_slot(slot)
    unpack(1, range(NARROW, held))

    def member_step(group):
        def step(member, carry):
            slot = group * held + member
            prepare(slot)
            compute(slot, member)

            @pl.when(slot < early)
            def _():
                send_slot(slot)

            return carry

        return step

    lax.fori_loop(NARROW, held, member_step(0), 0)

    def group_step(group, carry):
        unpack(group + 1, range(held))
        lax.fori_loop(0, held, member_step(group), 0)
        return carry

    lax.fori_loop(1, slots // held, group_step, 0)

    pairs_group = 1 + chunks
    for_peers(lambda peer: copy(pair_row, pair_rows.at[me], pairs_group, peer).start())
    pair_rows[me] = pair_row[...]

    def chunk_step(index, carry):
        send_chunk(index)
        return carry

    lax.fori_loop(0, chunks, chunk_step, 0)

    others = pl.ds(0, devices - 1)
    whole = lambda ref: ref.at[others, pl.ds(0, early)]
    part = lambda ref, index: ref.at[others, pl.ds(early, slots - early), pl.ds(index * chunk, chunk), :]

    def wait_bytes(ref, sem):
        pltpu.make_async_copy(ref, ref, sem).wait()

    wait_bytes(pair_rows.at[others], recv_sem.at[pairs_group])

    def column_step(device, carry):
        row = pair_rows[device].astype(jnp.float32)
        rows = jnp.broadcast_to(row, (slots, row.shape[-1]))
        own = lax.broadcasted_iota(jnp.int32, rows.shape, 0) == lax.broadcasted_iota(jnp.int32, rows.shape, 1)
        column = jnp.sum(jnp.where(own, rows, 0.0), axis=1, keepdims=True)
        at = pl.ds(pl.multiple_of(device * slots, slots), slots)
        pair_columns[at, :] = jnp.broadcast_to(column, (slots, pair_columns.shape[1]))
        return carry

    lax.fori_loop(0, devices, column_step, 0)
    step = 64
    lane = lax.broadcasted_iota(jnp.int32, (step, total), 1)
    for low in range(0, total, step):
        pairs = pair_columns[low:low + step, :1].astype(jnp.int32)
        place[0, low:low + step, :] = (pairs == lane).astype(jnp.float32).astype(jnp.bfloat16)
        place[1, low:low + step, :] = (total - 1 - pairs == lane).astype(jnp.float32).astype(jnp.bfloat16)

    wait_bytes(whole(incoming), recv_sem.at[0])
    flat = recv.reshape(devices * slots * band, lanes)

    def place_step(index, carry):
        wait_bytes(part(incoming, index), recv_sem.at[1 + index])
        for i in range(chunk):
            row = index * chunk + i
            values = flat[pl.ds(row, total, stride=band), :].T
            high = values.astype(jnp.bfloat16)
            low = (values - high.astype(jnp.float32)).astype(jnp.bfloat16)
            for w in range(2):
                at = slice(i * columns, (i + 1) * columns)
                high_rows[w, at, :] = high[w * columns:(w + 1) * columns]
                low_rows[w, at, :] = low[w * columns:(w + 1) * columns]
        for w in range(2):
            placed = jnp.dot(high_rows[w], place[w], preferred_element_type=jnp.float32)
            placed += jnp.dot(low_rows[w], place[w], preferred_element_type=jnp.float32)
            for i in range(chunk):
                row = index * chunk + i
                to = row + side * (band - 1 - 2 * row)
                out_ref[to, :, w * total:(w + 1) * total] = placed[i * columns:(i + 1) * columns]
        return carry

    lax.fori_loop(0, chunks, place_step, 0)

    wait_bytes(whole(outgoing), send_sem.at[0])

    def drain_step(index, carry):
        wait_bytes(part(outgoing, index), send_sem.at[1 + index])
        return carry

    lax.fori_loop(0, chunks, drain_step, 0)
    wait_bytes(pair_rows.at[others], send_sem.at[pairs_group])


def shards(coeffs, legendre, assign):
    devices = lax.axis_size("ma")
    slots, columns, width = coeffs.shape
    lat_half = legendre.shape[1]
    band = 2 * lat_half // devices
    total = devices * slots
    lanes = 2 * columns
    chunk = min(CHUNK_ROWS, band)
    early = max(slots // EARLY_PART, 1)
    groups = 2 + band // chunk
    held = min(8, slots)
    main = width // SPAN * SPAN
    return pl.pallas_call(
        functools.partial(synthesis_kernel, devices=devices, early=early, chunk=chunk),
        out_shape=pltpu.VMEM((band, columns, 2 * total), jnp.float32),
        in_specs=[
            pl.BlockSpec(memory_space=pltpu.SMEM),
            pl.BlockSpec(memory_space=pl.ANY),
            pl.BlockSpec(memory_space=pl.ANY),
        ],
        out_specs=pl.BlockSpec(memory_space=pltpu.VMEM),
        scratch_shapes=[
            pltpu.VMEM((BUFFERS, columns, width), jnp.bfloat16),
            pltpu.VMEM((LOADS, SPAN, held, lat_half), jnp.bfloat16),
            pltpu.VMEM((width - main, slots, lat_half), jnp.bfloat16),
            pltpu.VMEM((width - main, slots, lat_half), jnp.float32),
            pltpu.VMEM((lat_half // 128, SPAN * held, 128), jnp.float32),
            pltpu.VMEM((held, main, lat_half), jnp.bfloat16),
            pltpu.VMEM((4 * columns, main), jnp.bfloat16),
            pltpu.VMEM((devices, slots * band, lanes), jnp.float32),
            pltpu.VMEM((devices, slots * band, lanes), jnp.float32),
            pltpu.VMEM((1, lanes), jnp.int32),
            pltpu.VMEM((devices, 1, lanes), jnp.int32),
            pltpu.VMEM((total, lanes), jnp.float32),
            pltpu.VMEM((2, total, total), jnp.bfloat16),
            pltpu.VMEM((2, chunk * columns, total), jnp.bfloat16),
            pltpu.VMEM((2, chunk * columns, total), jnp.bfloat16),
            pltpu.SemaphoreType.DMA((BUFFERS,)),
            pltpu.SemaphoreType.DMA((LOADS,)),
            pltpu.SemaphoreType.DMA,
            pltpu.SemaphoreType.DMA((groups,)),
            pltpu.SemaphoreType.DMA((groups,)),
        ],
        compiler_params=pltpu.CompilerParams(
            collective_id=0, has_side_effects=True, vmem_limit_bytes=50 * 1024 * 1024
        ),
        name="synthesis",
    )(assign, coeffs, legendre.transpose(2, 0, 1))


def solution(mesh):
    return jax.shard_map(
        shards,
        mesh=mesh,
        in_specs=(P("ma", "af", None), P("ma", None, None), P("ma")),
        out_specs=P("ma", "af", None),
        check_vma=False,
    )
```

```python
import functools

import jax
import jax.numpy as jnp
from jax import lax
from jax.experimental import pallas as pl
from jax.experimental.pallas import tpu as pltpu
from jax.sharding import PartitionSpec as P

MESH = pl.DeviceIdType.MESH
BUFFERS = 3
LOADS = 8
NARROW = 2
SPAN = 256
CHUNK_ROWS = 2
EARLY_PART = 2


def mask_groups(first_len, coeff_ref, out_ref):
    columns = coeff_ref.shape[0]
    width = out_ref.shape[1]
    pack = 16
    entry = lax.broadcasted_iota(jnp.int32, (pack, width), 1)
    first = entry < first_len
    odd_gap = (jnp.where(first, entry, entry - first_len) & 1) == 1
    sign = jnp.where(odd_gap, -1.0, 1.0)
    scales = [
        jnp.where(first, 1.0, 0.0),
        jnp.where(first, 0.0, 1.0),
        jnp.where(first, sign, 0.0),
        jnp.where(first, 0.0, sign),
    ]
    scales = [scale.astype(out_ref.dtype) for scale in scales]
    for low in range(0, columns, pack):
        values = coeff_ref[low:low + pack, :width]
        for index, scale in enumerate(scales):
            at = index * columns + low
            out_ref[at:at + pack, :] = values * scale


def last_entries(first_len, coeff_ref, row_of, start):
    columns, width = coeff_ref.shape
    total = 0.0
    for entry in range(start, width):
        first = entry < first_len
        gap = jnp.where(first, entry, entry - first_len)
        sign = jnp.where((gap & 1) == 1, -1.0, 1.0)
        outer = coeff_ref[:, entry:entry + 1].astype(jnp.float32) * row_of(entry - start)
        kinds = [jnp.where(first, 1.0, 0.0), jnp.where(first, 0.0, 1.0)]
        kinds += [kind * sign for kind in kinds]
        total += jnp.concatenate([outer * kind for kind in kinds], axis=0)
    return total


def place_rows(flat, place, high_rows, low_rows, first, count, band, store):
    columns = high_rows.shape[1] // count
    total = place.shape[1]

    def split_row(i, carry):
        values = flat[pl.ds(first + i, total, stride=band), :].T
        high = values.astype(jnp.bfloat16)
        low = (values - high.astype(jnp.float32)).astype(jnp.bfloat16)
        at = pl.ds(pl.multiple_of(i * columns, columns), columns)
        for w in range(2):
            high_rows[w, at, :] = high[w * columns:(w + 1) * columns]
            low_rows[w, at, :] = low[w * columns:(w + 1) * columns]
        return carry

    lax.fori_loop(0, count, split_row, 0)
    for w in range(2):
        placed = jnp.dot(high_rows[w], place[w], preferred_element_type=jnp.float32)
        placed += jnp.dot(low_rows[w], place[w], preferred_element_type=jnp.float32)
        for i in range(count):
            store(i, w, placed[i * columns:(i + 1) * columns])


def synthesis_kernel(
    assign_ref, coeffs_ref, legendre_ref, out_ref, recv, place,
    coeff_buf, legendre_buf, rest, rest_wide, wide, functions, groups, send, pair_row, pair_rows, pair_columns,
    high_rows, low_rows,
    coeff_sem, span_sem, rest_sem, send_sem, recv_sem, *, devices, early, chunk,
):
    me = lax.axis_index("ma")
    half = devices // 2
    side = lax.div(me, half)
    slots, columns, width = coeffs_ref.shape
    lat_half = legendre_ref.shape[2]
    held = functions.shape[0]
    spans = width // SPAN
    turns = 1 + slots // held
    parts = held // NARROW
    share = SPAN // parts
    lanes = 2 * columns
    band = send.shape[1] // slots
    total = devices * slots
    chunks = band // chunk
    by_slot = (devices, slots, band, lanes)
    outgoing = send.reshape(by_slot)
    incoming = recv.reshape(by_slot)

    def coeff_load(slot):
        buf = lax.rem(slot, BUFFERS)
        return pltpu.make_async_copy(coeffs_ref.at[slot], coeff_buf.at[buf], coeff_sem.at[buf])

    def span_load(index):
        buf = lax.rem(index, LOADS)
        rows = pl.ds(lax.rem(index, spans) * SPAN, SPAN)
        group = jnp.maximum(index // spans - 1, 0)
        source = legendre_ref.at[rows, pl.ds(pl.multiple_of(group * held, held), held), :]
        return pltpu.make_async_copy(source, legendre_buf.at[buf], span_sem.at[buf])

    def narrow_loads(span):
        buf = lax.rem(span, LOADS)
        return [
            pltpu.make_async_copy(
                legendre_ref.at[pl.ds(span * SPAN + part * share, share), pl.ds(0, NARROW), :],
                legendre_buf.at[buf, pl.ds(0, share), pl.ds(part * NARROW, NARROW), :],
                span_sem.at[buf],
            )
            for part in range(parts)
        ]

    def widen(buf, rows):
        for low in range(0, lat_half, 128):
            block = legendre_buf[buf, :rows, :, low:low + 128].astype(jnp.float32)
            wide[low // 128, :rows * held] = block.reshape(rows * held, 128)

    def pick(member, at, first, rows):
        for low in range(0, lat_half, 128):
            block = wide[low // 128, pl.ds(first, rows, stride=held), :]
            functions[member, at, low:low + 128] = block.astype(functions.dtype)

    def unpack_narrow():
        def span_step(span, carry):
            buf = lax.rem(span, LOADS)
            landed = legendre_buf.at[buf, pl.ds(0, share)]
            pltpu.make_async_copy(landed, landed, span_sem.at[buf]).wait()
            widen(buf, share)
            later = span + LOADS

            @pl.when(later < spans)
            def _():
                for load in narrow_loads(later):
                    load.start()

            @pl.when(later >= spans)
            def _():
                span_load(later).start()

            for member in range(NARROW):
                for part in range(parts):
                    at = pl.ds(pl.multiple_of(span * SPAN + part * share, share), share)
                    pick(member, at, part * NARROW + member, share)
            return carry

        lax.fori_loop(0, spans, span_step, 0)

    def unpack(turn, members):
        def span_step(span, carry):
            index = turn * spans + span
            span_load(index).wait()
            buf = lax.rem(index, LOADS)
            widen(buf, SPAN)

            @pl.when(index + LOADS < turns * spans)
            def _():
                span_load(index + LOADS).start()

            at = pl.ds(pl.multiple_of(span * SPAN, SPAN), SPAN)
            for member in members:
                pick(member, at, member, SPAN)
            return carry

        lax.fori_loop(0, spans, span_step, 0)

    def meet(k):
        place_in_half = lax.rem(me, half)
        if half & (half - 1):
            return lax.rem(place_in_half + k, half)
        partner = 0
        for bit in [2 ** n for n in range(half.bit_length() - 1)]:
            partner += lax.rem(lax.div(place_in_half, bit) + lax.div(k, bit), 2) * bit
        return partner

    def for_peers(act):
        def across(k, carry):
            act((1 - side) * half + meet(k))
            return carry

        def within(k, carry):
            act(side * half + meet(k))
            return carry

        lax.fori_loop(0, half, across, 0)
        lax.fori_loop(1, half, within, 0)

    def copy(source, target, group, peer):
        return pltpu.make_async_remote_copy(
            src_ref=source,
            dst_ref=target,
            send_sem=send_sem.at[group],
            recv_sem=recv_sem.at[group],
            device_id={"ma": peer},
            device_id_type=MESH,
        )

    def prepare(slot):
        coeff_load(slot).wait()
        buf = lax.rem(slot, BUFFERS)
        pair = assign_ref[slot]
        lane = lax.broadcasted_iota(jnp.int32, pair_row.shape, 1)
        pair_row[...] = jnp.where(lane == slot, pair, pair_row[...])
        first_len = width - 1 - pair
        mask_groups(first_len, coeff_buf.at[buf], groups)

    def compute(slot, member):
        buf = lax.rem(slot, BUFFERS)
        first_len = width - 1 - assign_ref[slot]
        value = jnp.dot(groups[...], functions[member], preferred_element_type=jnp.float32)
        value += last_entries(first_len, coeff_buf.at[buf], lambda n: rest_wide[n, pl.ds(slot, 1), :], spans * SPAN)
        value = value.T
        at = pl.ds(pl.multiple_of(slot * band, band), band)
        for block in range(half):
            rows = slice(block * band, (block + 1) * band)
            send[block, at, :] = value[rows, :lanes]
            send[devices - 1 - block, at, :] = value[rows, lanes:]
        recv[me, at, :] = send[me, at, :]

        @pl.when(slot + BUFFERS < slots)
        def _():
            coeff_load(slot + BUFFERS).start()

    def send_slot(slot):
        for_peers(lambda peer: copy(outgoing.at[peer, slot], incoming.at[me, slot], 0, peer).start())

    def late(ref, device, first_row):
        return ref.at[device, pl.ds(early, slots - early), pl.ds(first_row, chunk), :]

    def send_chunk(index):
        row = index * chunk
        for_peers(lambda peer: copy(late(outgoing, peer, row), late(incoming, me, row), 1 + index, peer).start())

    coeff_load(0).start()
    rest_load = pltpu.make_async_copy(legendre_ref.at[pl.ds(spans * SPAN, width - spans * SPAN)], rest, rest_sem)
    rest_load.start()
    for index in range(min(LOADS, spans)):
        for load in narrow_loads(index):
            load.start()
    for index in range(spans, LOADS):
        span_load(index).start()
    for slot in range(1, min(BUFFERS, slots)):
        coeff_load(slot).start()
    barrier = pltpu.get_barrier_semaphore()
    for_peers(lambda peer: pl.semaphore_signal(barrier, inc=1, device_id={"ma": peer}, device_id_type=MESH))
    pair_row[...] = jnp.zeros_like(pair_row)
    prepare(0)
    unpack_narrow()
    rest_load.wait()
    rest_wide[...] = rest[...].astype(jnp.float32)
    compute(0, 0)
    pl.semaphore_wait(barrier, devices - 1)
    send_slot(0)
    for slot in range(1, NARROW):
        prepare(slot)
        compute(slot, slot)
        send_slot(slot)
    unpack(1, range(NARROW, held))

    def member_step(group):
        def step(member, carry):
            slot = group * held + member
            prepare(slot)
            compute(slot, member)

            @pl.when(slot < early)
            def _():
                send_slot(slot)

            return carry

        return step

    lax.fori_loop(NARROW, held, member_step(0), 0)

    def group_step(group, carry):
        unpack(group + 1, range(held))
        lax.fori_loop(0, held, member_step(group), 0)
        return carry

    lax.fori_loop(1, slots // held, group_step, 0)

    pairs_group = 1 + chunks
    for_peers(lambda peer: copy(pair_row, pair_rows.at[me], pairs_group, peer).start())
    pair_rows[me] = pair_row[...]

    def chunk_step(index, carry):
        send_chunk(index)
        return carry

    lax.fori_loop(0, chunks, chunk_step, 0)

    others = pl.ds(0, devices - 1)
    whole = lambda ref: ref.at[others, pl.ds(0, early)]
    part = lambda ref, index: ref.at[others, pl.ds(early, slots - early), pl.ds(index * chunk, chunk), :]

    def wait_bytes(ref, sem):
        pltpu.make_async_copy(ref, ref, sem).wait()

    wait_bytes(pair_rows.at[others], recv_sem.at[pairs_group])

    def column_step(device, carry):
        row = pair_rows[device].astype(jnp.float32)
        rows = jnp.broadcast_to(row, (slots, row.shape[-1]))
        own = lax.broadcasted_iota(jnp.int32, rows.shape, 0) == lax.broadcasted_iota(jnp.int32, rows.shape, 1)
        column = jnp.sum(jnp.where(own, rows, 0.0), axis=1, keepdims=True)
        at = pl.ds(pl.multiple_of(device * slots, slots), slots)
        pair_columns[at, :] = jnp.broadcast_to(column, (slots, pair_columns.shape[1]))
        return carry

    lax.fori_loop(0, devices, column_step, 0)
    step = 64
    lane = lax.broadcasted_iota(jnp.int32, (step, total), 1)
    for low in range(0, total, step):
        pairs = pair_columns[low:low + step, :1].astype(jnp.int32)
        place[0, low:low + step, :] = (pairs == lane).astype(jnp.float32).astype(jnp.bfloat16)
        place[1, low:low + step, :] = (total - 1 - pairs == lane).astype(jnp.float32).astype(jnp.bfloat16)

    wait_bytes(whole(incoming), recv_sem.at[0])
    flat = recv.reshape(devices * slots * band, lanes)

    def place_step(index, carry):
        wait_bytes(part(incoming, index), recv_sem.at[1 + index])

        def store(i, w, values):
            row = index * chunk + i
            out_ref[row + side * (band - 1 - 2 * row), :, w * total:(w + 1) * total] = values

        place_rows(flat, place, high_rows, low_rows, index * chunk, chunk, band, store)
        return carry

    lax.fori_loop(0, chunks - 1, place_step, 0)
    wait_bytes(part(incoming, chunks - 1), recv_sem.at[chunks])

    wait_bytes(whole(outgoing), send_sem.at[0])

    def drain_step(index, carry):
        wait_bytes(part(outgoing, index), send_sem.at[1 + index])
        return carry

    lax.fori_loop(0, chunks, drain_step, 0)
    wait_bytes(pair_rows.at[others], send_sem.at[pairs_group])


def deliver_kernel(placed_ref, recv, place, out_ref, last, high_rows, low_rows, sems, *, devices):
    side = lax.div(lax.axis_index("ma"), devices // 2)
    band = out_ref.shape[0]
    count, _, total = last.shape
    total //= 2
    ready = pl.ds(side * count, band - count)
    bulk = pltpu.make_async_copy(placed_ref.at[ready], out_ref.at[ready], sems.at[0])
    bulk.start()
    flat = recv.reshape(total * band, recv.shape[-1])

    def store(i, w, values):
        to = i + side * (count - 1 - 2 * i)
        last[to, :, w * total:(w + 1) * total] = values

    place_rows(flat, place, high_rows, low_rows, band - count, count, band, store)
    tail = pltpu.make_async_copy(last, out_ref.at[pl.ds((1 - side) * (band - count), count)], sems.at[1])
    tail.start()
    bulk.wait()
    tail.wait()


def shards(coeffs, legendre, assign):
    devices = lax.axis_size("ma")
    slots, columns, width = coeffs.shape
    lat_half = legendre.shape[1]
    band = 2 * lat_half // devices
    total = devices * slots
    lanes = 2 * columns
    chunk = min(CHUNK_ROWS, band)
    early = max(slots // EARLY_PART, 1)
    groups = 2 + band // chunk
    held = min(8, slots)
    main = width // SPAN * SPAN
    placed, received, place = pl.pallas_call(
        functools.partial(synthesis_kernel, devices=devices, early=early, chunk=chunk),
        out_shape=[
            pltpu.VMEM((band, columns, 2 * total), jnp.float32),
            pltpu.VMEM((devices, slots * band, lanes), jnp.float32),
            pltpu.VMEM((2, total, total), jnp.bfloat16),
        ],
        in_specs=[
            pl.BlockSpec(memory_space=pltpu.SMEM),
            pl.BlockSpec(memory_space=pl.ANY),
            pl.BlockSpec(memory_space=pl.ANY),
        ],
        out_specs=[pl.BlockSpec(memory_space=pltpu.VMEM)] * 3,
        scratch_shapes=[
            pltpu.VMEM((BUFFERS, columns, width), jnp.bfloat16),
            pltpu.VMEM((LOADS, SPAN, held, lat_half), jnp.bfloat16),
            pltpu.VMEM((width - main, slots, lat_half), jnp.bfloat16),
            pltpu.VMEM((width - main, slots, lat_half), jnp.float32),
            pltpu.VMEM((lat_half // 128, SPAN * held, 128), jnp.float32),
            pltpu.VMEM((held, main, lat_half), jnp.bfloat16),
            pltpu.VMEM((4 * columns, main), jnp.bfloat16),
            pltpu.VMEM((devices, slots * band, lanes), jnp.float32),
            pltpu.VMEM((1, lanes), jnp.int32),
            pltpu.VMEM((devices, 1, lanes), jnp.int32),
            pltpu.VMEM((total, lanes), jnp.float32),
            pltpu.VMEM((2, chunk * columns, total), jnp.bfloat16),
            pltpu.VMEM((2, chunk * columns, total), jnp.bfloat16),
            pltpu.SemaphoreType.DMA((BUFFERS,)),
            pltpu.SemaphoreType.DMA((LOADS,)),
            pltpu.SemaphoreType.DMA,
            pltpu.SemaphoreType.DMA((groups,)),
            pltpu.SemaphoreType.DMA((groups,)),
        ],
        compiler_params=pltpu.CompilerParams(
            collective_id=0, has_side_effects=True, vmem_limit_bytes=40 * 1024 * 1024
        ),
        name="synthesis",
    )(assign, coeffs, legendre.transpose(2, 0, 1))
    return pl.pallas_call(
        functools.partial(deliver_kernel, devices=devices),
        out_shape=jax.ShapeDtypeStruct((band, columns, 2 * total), jnp.float32),
        in_specs=[pl.BlockSpec(memory_space=pltpu.VMEM)] * 3,
        out_specs=pl.BlockSpec(memory_space=pl.ANY),
        scratch_shapes=[
            pltpu.VMEM((chunk, columns, 2 * total), jnp.float32),
            pltpu.VMEM((2, chunk * columns, total), jnp.bfloat16),
            pltpu.VMEM((2, chunk * columns, total), jnp.bfloat16),
            pltpu.SemaphoreType.DMA((2,)),
        ],
        compiler_params=pltpu.CompilerParams(vmem_limit_bytes=8 * 1024 * 1024),
        name="deliver",
    )(placed, received, place)


def solution(mesh):
    return jax.shard_map(
        shards,
        mesh=mesh,
        in_specs=(P("ma", "af", None), P("ma", None, None), P("ma")),
        out_specs=P("ma", "af", None),
        check_vma=False,
    )
```

```python
import functools

import jax
import jax.numpy as jnp
from jax import lax
from jax.experimental import pallas as pl
from jax.experimental.pallas import tpu as pltpu
from jax.sharding import PartitionSpec as P

MESH = pl.DeviceIdType.MESH
BUFFERS = 3
LOADS = 8
NARROW = 2
SPAN = 256
CHUNK_ROWS = 4
EARLY_PART = 4


def mask_groups(first_len, coeff_ref, out_ref):
    columns = coeff_ref.shape[0]
    width = out_ref.shape[1]
    pack = 16
    entry = lax.broadcasted_iota(jnp.int32, (pack, width), 1)
    first = entry < first_len
    odd_gap = (jnp.where(first, entry, entry - first_len) & 1) == 1
    sign = jnp.where(odd_gap, -1.0, 1.0)
    scales = [
        jnp.where(first, 1.0, 0.0),
        jnp.where(first, 0.0, 1.0),
        jnp.where(first, sign, 0.0),
        jnp.where(first, 0.0, sign),
    ]
    scales = [scale.astype(out_ref.dtype) for scale in scales]
    for low in range(0, columns, pack):
        values = coeff_ref[low:low + pack, :width]
        for index, scale in enumerate(scales):
            at = index * columns + low
            out_ref[at:at + pack, :] = values * scale


def last_entries(first_len, coeff_ref, row_of, start):
    columns, width = coeff_ref.shape
    total = 0.0
    for entry in range(start, width):
        first = entry < first_len
        gap = jnp.where(first, entry, entry - first_len)
        sign = jnp.where((gap & 1) == 1, -1.0, 1.0)
        outer = coeff_ref[:, entry:entry + 1].astype(jnp.float32) * row_of(entry - start)
        kinds = [jnp.where(first, 1.0, 0.0), jnp.where(first, 0.0, 1.0)]
        kinds += [kind * sign for kind in kinds]
        total += jnp.concatenate([outer * kind for kind in kinds], axis=0)
    return total


def place_rows(flat, place, high_rows, low_rows, first, count, band, store):
    columns = high_rows.shape[1] // count
    total = place.shape[1]

    def split_row(i, carry):
        values = flat[pl.ds(first + i, total, stride=band), :].T
        high = values.astype(jnp.bfloat16)
        low = (values - high.astype(jnp.float32)).astype(jnp.bfloat16)
        at = pl.ds(pl.multiple_of(i * columns, columns), columns)
        for w in range(2):
            high_rows[w, at, :] = high[w * columns:(w + 1) * columns]
            low_rows[w, at, :] = low[w * columns:(w + 1) * columns]
        return carry

    lax.fori_loop(0, count, split_row, 0)
    for w in range(2):
        placed = jnp.dot(high_rows[w], place[w], preferred_element_type=jnp.float32)
        placed += jnp.dot(low_rows[w], place[w], preferred_element_type=jnp.float32)
        for i in range(count):
            store(i, w, placed[i * columns:(i + 1) * columns])


def synthesis_kernel(
    assign_hbm, coeffs_ref, legendre_ref, out_ref, recv, place,
    assign_ref, coeff_buf, legendre_buf, rest, rest_wide, wide, functions, groups, send, pair_row, pair_rows, pair_columns,
    high_rows, low_rows,
    assign_sem, coeff_sem, span_sem, rest_sem, send_sem, recv_sem, *, devices, early, chunk,
):
    me = lax.axis_index("ma")
    half = devices // 2
    side = lax.div(me, half)
    slots, columns, width = coeffs_ref.shape
    lat_half = legendre_ref.shape[2]
    held = functions.shape[0]
    spans = width // SPAN
    turns = 1 + slots // held
    parts = held // NARROW
    share = SPAN // parts
    lanes = 2 * columns
    band = send.shape[1] // slots
    total = devices * slots
    chunks = band // chunk
    by_slot = (devices, slots, band, lanes)
    outgoing = send.reshape(by_slot)
    incoming = recv.reshape(by_slot)

    def coeff_load(slot):
        buf = lax.rem(slot, BUFFERS)
        return pltpu.make_async_copy(coeffs_ref.at[slot], coeff_buf.at[buf], coeff_sem.at[buf])

    def span_load(index):
        buf = lax.rem(index, LOADS)
        rows = pl.ds(lax.rem(index, spans) * SPAN, SPAN)
        group = jnp.maximum(index // spans - 1, 0)
        source = legendre_ref.at[rows, pl.ds(pl.multiple_of(group * held, held), held), :]
        return pltpu.make_async_copy(source, legendre_buf.at[buf], span_sem.at[buf])

    def narrow_loads(span):
        buf = lax.rem(span, LOADS)
        return [
            pltpu.make_async_copy(
                legendre_ref.at[pl.ds(span * SPAN + part * share, share), pl.ds(0, NARROW), :],
                legendre_buf.at[buf, pl.ds(0, share), pl.ds(part * NARROW, NARROW), :],
                span_sem.at[buf],
            )
            for part in range(parts)
        ]

    def widen(buf, rows):
        for low in range(0, lat_half, 128):
            block = legendre_buf[buf, :rows, :, low:low + 128].astype(jnp.float32)
            wide[low // 128, :rows * held] = block.reshape(rows * held, 128)

    def pick(member, at, first, rows):
        for low in range(0, lat_half, 128):
            block = wide[low // 128, pl.ds(first, rows, stride=held), :]
            functions[member, at, low:low + 128] = block.astype(functions.dtype)

    def unpack_narrow():
        def span_step(span, carry):
            buf = lax.rem(span, LOADS)
            landed = legendre_buf.at[buf, pl.ds(0, share)]
            pltpu.make_async_copy(landed, landed, span_sem.at[buf]).wait()
            widen(buf, share)
            later = span + LOADS

            @pl.when(later < spans)
            def _():
                for load in narrow_loads(later):
                    load.start()

            @pl.when(later >= spans)
            def _():
                span_load(later).start()

            for member in range(NARROW):
                for part in range(parts):
                    at = pl.ds(pl.multiple_of(span * SPAN + part * share, share), share)
                    pick(member, at, part * NARROW + member, share)
            return carry

        lax.fori_loop(0, spans, span_step, 0)

    def unpack(turn, members):
        def span_step(span, carry):
            index = turn * spans + span
            span_load(index).wait()
            buf = lax.rem(index, LOADS)
            widen(buf, SPAN)

            @pl.when(index + LOADS < turns * spans)
            def _():
                span_load(index + LOADS).start()

            at = pl.ds(pl.multiple_of(span * SPAN, SPAN), SPAN)
            for member in members:
                pick(member, at, member, SPAN)
            return carry

        lax.fori_loop(0, spans, span_step, 0)

    def meet(k):
        place_in_half = lax.rem(me, half)
        if half & (half - 1):
            return lax.rem(place_in_half + k, half)
        partner = 0
        for bit in [2 ** n for n in range(half.bit_length() - 1)]:
            partner += lax.rem(lax.div(place_in_half, bit) + lax.div(k, bit), 2) * bit
        return partner

    def for_peers(act):
        def across(k, carry):
            act((1 - side) * half + meet(k))
            return carry

        def within(k, carry):
            act(side * half + meet(k))
            return carry

        lax.fori_loop(0, half, across, 0)
        lax.fori_loop(1, half, within, 0)

    def copy(source, target, group, peer):
        return pltpu.make_async_remote_copy(
            src_ref=source,
            dst_ref=target,
            send_sem=send_sem.at[group],
            recv_sem=recv_sem.at[group],
            device_id={"ma": peer},
            device_id_type=MESH,
        )

    def prepare(slot):
        coeff_load(slot).wait()
        buf = lax.rem(slot, BUFFERS)
        pair = assign_ref[slot]
        lane = lax.broadcasted_iota(jnp.int32, pair_row.shape, 1)
        pair_row[...] = jnp.where(lane == slot, pair, pair_row[...])
        first_len = width - 1 - pair
        mask_groups(first_len, coeff_buf.at[buf], groups)

    def compute(slot, member):
        buf = lax.rem(slot, BUFFERS)
        first_len = width - 1 - assign_ref[slot]
        value = jnp.dot(groups[...], functions[member], preferred_element_type=jnp.float32)
        value += last_entries(first_len, coeff_buf.at[buf], lambda n: rest_wide[n, pl.ds(slot, 1), :], spans * SPAN)
        value = value.T
        at = pl.ds(pl.multiple_of(slot * band, band), band)
        for block in range(half):
            rows = slice(block * band, (block + 1) * band)
            send[block, at, :] = value[rows, :lanes]
            send[devices - 1 - block, at, :] = value[rows, lanes:]
        recv[me, at, :] = send[me, at, :]

        @pl.when(slot + BUFFERS < slots)
        def _():
            coeff_load(slot + BUFFERS).start()

    def send_slot(slot):
        for_peers(lambda peer: copy(outgoing.at[peer, slot], incoming.at[me, slot], 0, peer).start())

    def late(ref, device, first_row):
        return ref.at[device, pl.ds(early, slots - early), pl.ds(first_row, chunk), :]

    def send_chunk(index):
        row = index * chunk
        for_peers(lambda peer: copy(late(outgoing, peer, row), late(incoming, me, row), 1 + index, peer).start())

    barrier = pltpu.get_barrier_semaphore()
    for_peers(lambda peer: pl.semaphore_signal(barrier, inc=1, device_id={"ma": peer}, device_id_type=MESH))
    assign_load = pltpu.make_async_copy(assign_hbm, assign_ref, assign_sem)
    assign_load.start()
    coeff_load(0).start()
    rest_load = pltpu.make_async_copy(legendre_ref.at[pl.ds(spans * SPAN, width - spans * SPAN)], rest, rest_sem)
    rest_load.start()
    for index in range(min(LOADS, spans)):
        for load in narrow_loads(index):
            load.start()
    for index in range(spans, LOADS):
        span_load(index).start()
    for slot in range(1, min(BUFFERS, slots)):
        coeff_load(slot).start()
    pair_row[...] = jnp.zeros_like(pair_row)
    assign_load.wait()
    prepare(0)
    unpack_narrow()
    rest_load.wait()
    rest_wide[...] = rest[...].astype(jnp.float32)
    compute(0, 0)
    pl.semaphore_wait(barrier, devices - 1)
    send_slot(0)
    for slot in range(1, NARROW):
        prepare(slot)
        compute(slot, slot)
        send_slot(slot)
    unpack(1, range(NARROW, held))

    def member_step(group):
        def step(member, carry):
            slot = group * held + member
            prepare(slot)
            compute(slot, member)

            @pl.when(slot < early)
            def _():
                send_slot(slot)

            return carry

        return step

    lax.fori_loop(NARROW, held, member_step(0), 0)

    def group_step(group, carry):
        unpack(group + 1, range(held))
        lax.fori_loop(0, held, member_step(group), 0)
        return carry

    lax.fori_loop(1, slots // held, group_step, 0)

    pairs_group = 1 + chunks
    for_peers(lambda peer: copy(pair_row, pair_rows.at[me], pairs_group, peer).start())
    pair_rows[me] = pair_row[...]

    def chunk_step(index, carry):
        send_chunk(index)
        return carry

    lax.fori_loop(0, chunks, chunk_step, 0)

    others = pl.ds(0, devices - 1)
    whole = lambda ref: ref.at[others, pl.ds(0, early)]
    part = lambda ref, index: ref.at[others, pl.ds(early, slots - early), pl.ds(index * chunk, chunk), :]

    def wait_bytes(ref, sem):
        pltpu.make_async_copy(ref, ref, sem).wait()

    wait_bytes(pair_rows.at[others], recv_sem.at[pairs_group])

    def column_step(device, carry):
        row = pair_rows[device].astype(jnp.float32)
        rows = jnp.broadcast_to(row, (slots, row.shape[-1]))
        own = lax.broadcasted_iota(jnp.int32, rows.shape, 0) == lax.broadcasted_iota(jnp.int32, rows.shape, 1)
        column = jnp.sum(jnp.where(own, rows, 0.0), axis=1, keepdims=True)
        at = pl.ds(pl.multiple_of(device * slots, slots), slots)
        pair_columns[at, :] = jnp.broadcast_to(column, (slots, pair_columns.shape[1]))
        return carry

    lax.fori_loop(0, devices, column_step, 0)
    step = 64
    lane = lax.broadcasted_iota(jnp.int32, (step, total), 1)
    for low in range(0, total, step):
        pairs = pair_columns[low:low + step, :1].astype(jnp.int32)
        place[0, low:low + step, :] = (pairs == lane).astype(jnp.float32).astype(jnp.bfloat16)
        place[1, low:low + step, :] = (total - 1 - pairs == lane).astype(jnp.float32).astype(jnp.bfloat16)

    wait_bytes(whole(incoming), recv_sem.at[0])
    flat = recv.reshape(devices * slots * band, lanes)

    def place_step(index, carry):
        wait_bytes(part(incoming, index), recv_sem.at[1 + index])

        def store(i, w, values):
            row = index * chunk + i
            out_ref[row + side * (band - 1 - 2 * row), :, w * total:(w + 1) * total] = values

        place_rows(flat, place, high_rows, low_rows, index * chunk, chunk, band, store)
        return carry

    lax.fori_loop(0, chunks - 1, place_step, 0)
    wait_bytes(part(incoming, chunks - 1), recv_sem.at[chunks])

    wait_bytes(whole(outgoing), send_sem.at[0])

    def drain_step(index, carry):
        wait_bytes(part(outgoing, index), send_sem.at[1 + index])
        return carry

    lax.fori_loop(0, chunks, drain_step, 0)
    wait_bytes(pair_rows.at[others], send_sem.at[pairs_group])


def deliver_kernel(placed_ref, recv, place, out_ref, last, high_rows, low_rows, sems, *, devices):
    side = lax.div(lax.axis_index("ma"), devices // 2)
    band = out_ref.shape[0]
    count, _, total = last.shape
    total //= 2
    ready = pl.ds(side * count, band - count)
    bulk = pltpu.make_async_copy(placed_ref.at[ready], out_ref.at[ready], sems.at[0])
    bulk.start()
    flat = recv.reshape(total * band, recv.shape[-1])

    def store(i, w, values):
        to = i + side * (count - 1 - 2 * i)
        last[to, :, w * total:(w + 1) * total] = values

    place_rows(flat, place, high_rows, low_rows, band - count, count, band, store)
    tail = pltpu.make_async_copy(last, out_ref.at[pl.ds((1 - side) * (band - count), count)], sems.at[1])
    tail.start()
    bulk.wait()
    tail.wait()


def shards(coeffs, legendre, assign):
    devices = lax.axis_size("ma")
    slots, columns, width = coeffs.shape
    lat_half = legendre.shape[1]
    band = 2 * lat_half // devices
    total = devices * slots
    lanes = 2 * columns
    chunk = min(CHUNK_ROWS, band)
    early = max(slots // EARLY_PART, NARROW)
    groups = 2 + band // chunk
    held = min(8, slots)
    main = width // SPAN * SPAN
    placed, received, place = pl.pallas_call(
        functools.partial(synthesis_kernel, devices=devices, early=early, chunk=chunk),
        out_shape=[
            pltpu.VMEM((band, columns, 2 * total), jnp.float32),
            pltpu.VMEM((devices, slots * band, lanes), jnp.float32),
            pltpu.VMEM((2, total, total), jnp.bfloat16),
        ],
        in_specs=[
            pl.BlockSpec(memory_space=pl.ANY),
            pl.BlockSpec(memory_space=pl.ANY),
            pl.BlockSpec(memory_space=pl.ANY),
        ],
        out_specs=[pl.BlockSpec(memory_space=pltpu.VMEM)] * 3,
        scratch_shapes=[
            pltpu.SMEM((slots,), jnp.int32),
            pltpu.VMEM((BUFFERS, columns, width), jnp.bfloat16),
            pltpu.VMEM((LOADS, SPAN, held, lat_half), jnp.bfloat16),
            pltpu.VMEM((width - main, slots, lat_half), jnp.bfloat16),
            pltpu.VMEM((width - main, slots, lat_half), jnp.float32),
            pltpu.VMEM((lat_half // 128, SPAN * held, 128), jnp.float32),
            pltpu.VMEM((held, main, lat_half), jnp.bfloat16),
            pltpu.VMEM((4 * columns, main), jnp.bfloat16),
            pltpu.VMEM((devices, slots * band, lanes), jnp.float32),
            pltpu.VMEM((1, lanes), jnp.int32),
            pltpu.VMEM((devices, 1, lanes), jnp.int32),
            pltpu.VMEM((total, lanes), jnp.float32),
            pltpu.VMEM((2, chunk * columns, total), jnp.bfloat16),
            pltpu.VMEM((2, chunk * columns, total), jnp.bfloat16),
            pltpu.SemaphoreType.DMA,
            pltpu.SemaphoreType.DMA((BUFFERS,)),
            pltpu.SemaphoreType.DMA((LOADS,)),
            pltpu.SemaphoreType.DMA,
            pltpu.SemaphoreType.DMA((groups,)),
            pltpu.SemaphoreType.DMA((groups,)),
        ],
        compiler_params=pltpu.CompilerParams(
            collective_id=0, has_side_effects=True, vmem_limit_bytes=40 * 1024 * 1024
        ),
        name="synthesis",
    )(assign, coeffs, legendre.transpose(2, 0, 1))
    return pl.pallas_call(
        functools.partial(deliver_kernel, devices=devices),
        out_shape=jax.ShapeDtypeStruct((band, columns, 2 * total), jnp.float32),
        in_specs=[pl.BlockSpec(memory_space=pltpu.VMEM)] * 3,
        out_specs=pl.BlockSpec(memory_space=pl.ANY),
        scratch_shapes=[
            pltpu.VMEM((chunk, columns, 2 * total), jnp.float32),
            pltpu.VMEM((2, chunk * columns, total), jnp.bfloat16),
            pltpu.VMEM((2, chunk * columns, total), jnp.bfloat16),
            pltpu.SemaphoreType.DMA((2,)),
        ],
        compiler_params=pltpu.CompilerParams(vmem_limit_bytes=8 * 1024 * 1024),
        name="deliver",
    )(placed, received, place)


def solution(mesh):
    return jax.shard_map(
        shards,
        mesh=mesh,
        in_specs=(P("ma", "af", None), P("ma", None, None), P("ma")),
        out_specs=P("ma", "af", None),
        check_vma=False,
    )
```

```python
import functools

import jax
import jax.numpy as jnp
from jax import lax
from jax.experimental import pallas as pl
from jax.experimental.pallas import tpu as pltpu
from jax.sharding import PartitionSpec as P

MESH = pl.DeviceIdType.MESH
BUFFERS = 3
LOADS = 8
NARROW = 2
SPAN = 256
CHUNK_ROWS = 4
EARLY_PART = 4


def mask_groups(first_len, coeff_ref, out_ref):
    columns = coeff_ref.shape[0]
    width = out_ref.shape[1]
    pack = 16
    entry = lax.broadcasted_iota(jnp.int32, (pack, width), 1)
    first = entry < first_len
    odd_gap = (jnp.where(first, entry, entry - first_len) & 1) == 1
    sign = jnp.where(odd_gap, -1.0, 1.0)
    scales = [
        jnp.where(first, 1.0, 0.0),
        jnp.where(first, 0.0, 1.0),
        jnp.where(first, sign, 0.0),
        jnp.where(first, 0.0, sign),
    ]
    scales = [scale.astype(out_ref.dtype) for scale in scales]
    for low in range(0, columns, pack):
        values = coeff_ref[low:low + pack, :width]
        for index, scale in enumerate(scales):
            at = index * columns + low
            out_ref[at:at + pack, :] = values * scale


def last_entries(first_len, coeff_ref, row_of, start):
    columns, width = coeff_ref.shape
    total = 0.0
    for entry in range(start, width):
        first = entry < first_len
        gap = jnp.where(first, entry, entry - first_len)
        sign = jnp.where((gap & 1) == 1, -1.0, 1.0)
        outer = coeff_ref[:, entry:entry + 1].astype(jnp.float32) * row_of(entry - start)
        kinds = [jnp.where(first, 1.0, 0.0), jnp.where(first, 0.0, 1.0)]
        kinds += [kind * sign for kind in kinds]
        total += jnp.concatenate([outer * kind for kind in kinds], axis=0)
    return total


def place_rows(flat, place, high_rows, low_rows, first, count, band, store):
    columns = high_rows.shape[1] // count
    total = place.shape[1]

    def split_row(i, carry):
        values = flat[pl.ds(first + i, total, stride=band), :].T
        high = values.astype(jnp.bfloat16)
        low = (values - high.astype(jnp.float32)).astype(jnp.bfloat16)
        at = pl.ds(pl.multiple_of(i * columns, columns), columns)
        for w in range(2):
            high_rows[w, at, :] = high[w * columns:(w + 1) * columns]
            low_rows[w, at, :] = low[w * columns:(w + 1) * columns]
        return carry

    lax.fori_loop(0, count, split_row, 0)
    for w in range(2):
        placed = jnp.dot(high_rows[w], place[w], preferred_element_type=jnp.float32)
        placed += jnp.dot(low_rows[w], place[w], preferred_element_type=jnp.float32)
        for i in range(count):
            store(i, w, placed[i * columns:(i + 1) * columns])


def synthesis_kernel(
    assign_hbm, coeffs_ref, legendre_ref, out_ref, recv, place,
    assign_ref, coeff_buf, legendre_buf, rest, rest_wide, wide, functions, groups, send, pair_row, pair_rows, pair_columns,
    high_rows, low_rows,
    assign_sem, coeff_sem, span_sem, rest_sem, send_sem, recv_sem, *, devices, early, chunk,
):
    me = lax.axis_index("ma")
    half = devices // 2
    side = lax.div(me, half)
    slots, columns, width = coeffs_ref.shape
    lat_half = legendre_ref.shape[2]
    held = functions.shape[0]
    spans = width // SPAN
    turns = 1 + slots // held
    parts = held // NARROW
    share = SPAN // parts
    lanes = 2 * columns
    band = send.shape[1] // slots
    total = devices * slots
    chunks = band // chunk
    by_slot = (devices, slots, band, lanes)
    outgoing = send.reshape(by_slot)
    incoming = recv.reshape(by_slot)

    def coeff_load(slot):
        buf = lax.rem(slot, BUFFERS)
        return pltpu.make_async_copy(coeffs_ref.at[slot], coeff_buf.at[buf], coeff_sem.at[buf])

    def span_load(index):
        buf = lax.rem(index, LOADS)
        rows = pl.ds(lax.rem(index, spans) * SPAN, SPAN)
        group = jnp.maximum(index // spans - 1, 0)
        source = legendre_ref.at[rows, pl.ds(pl.multiple_of(group * held, held), held), :]
        return pltpu.make_async_copy(source, legendre_buf.at[buf], span_sem.at[buf])

    def narrow_loads(span):
        buf = lax.rem(span, LOADS)
        return [
            pltpu.make_async_copy(
                legendre_ref.at[pl.ds(span * SPAN + part * share, share), pl.ds(0, NARROW), :],
                legendre_buf.at[buf, pl.ds(0, share), pl.ds(part * NARROW, NARROW), :],
                span_sem.at[buf],
            )
            for part in range(parts)
        ]

    def widen(buf, rows):
        for low in range(0, lat_half, 128):
            block = legendre_buf[buf, :rows, :, low:low + 128].astype(jnp.float32)
            wide[low // 128, :rows * held] = block.reshape(rows * held, 128)

    def pick(member, at, first, rows):
        for low in range(0, lat_half, 128):
            block = wide[low // 128, pl.ds(first, rows, stride=held), :]
            functions[member, at, low:low + 128] = block.astype(functions.dtype)

    def unpack_narrow():
        def span_step(span, carry):
            buf = lax.rem(span, LOADS)
            landed = legendre_buf.at[buf, pl.ds(0, share)]
            pltpu.make_async_copy(landed, landed, span_sem.at[buf]).wait()
            widen(buf, share)
            later = span + LOADS

            @pl.when(later < spans)
            def _():
                for load in narrow_loads(later):
                    load.start()

            @pl.when(later >= spans)
            def _():
                span_load(later).start()

            for member in range(NARROW):
                for part in range(parts):
                    at = pl.ds(pl.multiple_of(span * SPAN + part * share, share), share)
                    pick(member, at, part * NARROW + member, share)
            return carry

        lax.fori_loop(0, spans, span_step, 0)

    def unpack(turn, members):
        def span_step(span, carry):
            index = turn * spans + span
            span_load(index).wait()
            buf = lax.rem(index, LOADS)
            widen(buf, SPAN)

            @pl.when(index + LOADS < turns * spans)
            def _():
                span_load(index + LOADS).start()

            at = pl.ds(pl.multiple_of(span * SPAN, SPAN), SPAN)
            for member in members:
                pick(member, at, member, SPAN)
            return carry

        lax.fori_loop(0, spans, span_step, 0)

    def meet(k):
        place_in_half = lax.rem(me, half)
        if half & (half - 1):
            return lax.rem(place_in_half + k, half)
        partner = 0
        for bit in [2 ** n for n in range(half.bit_length() - 1)]:
            partner += lax.rem(lax.div(place_in_half, bit) + lax.div(k, bit), 2) * bit
        return partner

    def for_peers(act):
        def across(k, carry):
            act((1 - side) * half + meet(k))
            return carry

        def within(k, carry):
            act(side * half + meet(k))
            return carry

        lax.fori_loop(0, half, across, 0)
        lax.fori_loop(1, half, within, 0)

    def copy(source, target, group, peer):
        return pltpu.make_async_remote_copy(
            src_ref=source,
            dst_ref=target,
            send_sem=send_sem.at[group],
            recv_sem=recv_sem.at[group],
            device_id={"ma": peer},
            device_id_type=MESH,
        )

    def prepare(slot):
        coeff_load(slot).wait()
        buf = lax.rem(slot, BUFFERS)
        pair = assign_ref[slot]
        lane = lax.broadcasted_iota(jnp.int32, pair_row.shape, 1)
        pair_row[...] = jnp.where(lane == slot, pair, pair_row[...])
        first_len = width - 1 - pair
        mask_groups(first_len, coeff_buf.at[buf], groups)

    def compute(slot, member):
        buf = lax.rem(slot, BUFFERS)
        first_len = width - 1 - assign_ref[slot]
        value = jnp.dot(groups[...], functions[member], preferred_element_type=jnp.float32)
        value += last_entries(first_len, coeff_buf.at[buf], lambda n: rest_wide[n, pl.ds(slot, 1), :], spans * SPAN)
        value = value.T
        at = pl.ds(pl.multiple_of(slot * band, band), band)
        for block in range(half):
            rows = slice(block * band, (block + 1) * band)
            send[block, at, :] = value[rows, :lanes]
            send[devices - 1 - block, at, :] = value[rows, lanes:]
        recv[me, at, :] = send[me, at, :]

        @pl.when(slot + BUFFERS < slots)
        def _():
            coeff_load(slot + BUFFERS).start()

    def send_slot(slot):
        for_peers(lambda peer: copy(outgoing.at[peer, slot], incoming.at[me, slot], 0, peer).start())

    def late(ref, device, first_row):
        return ref.at[device, pl.ds(early, slots - early), pl.ds(first_row, chunk), :]

    def send_chunk(index):
        row = index * chunk
        for_peers(lambda peer: copy(late(outgoing, peer, row), late(incoming, me, row), 1 + index, peer).start())

    barrier = pltpu.get_barrier_semaphore()
    for_peers(lambda peer: pl.semaphore_signal(barrier, inc=1, device_id={"ma": peer}, device_id_type=MESH))
    assign_load = pltpu.make_async_copy(assign_hbm, assign_ref, assign_sem)
    assign_load.start()
    coeff_load(0).start()
    rest_load = pltpu.make_async_copy(legendre_ref.at[pl.ds(spans * SPAN, width - spans * SPAN)], rest, rest_sem)
    rest_load.start()
    for index in range(min(LOADS, spans)):
        for load in narrow_loads(index):
            load.start()
    for index in range(spans, LOADS):
        span_load(index).start()
    for slot in range(1, min(BUFFERS, slots)):
        coeff_load(slot).start()
    pair_row[...] = jnp.zeros_like(pair_row)
    assign_load.wait()
    prepare(0)
    unpack_narrow()
    rest_load.wait()
    rest_wide[...] = rest[...].astype(jnp.float32)
    compute(0, 0)
    pl.semaphore_wait(barrier, devices - 1)
    send_slot(0)
    for slot in range(1, NARROW):
        prepare(slot)
        compute(slot, slot)
        send_slot(slot)
    unpack(1, range(NARROW, held))

    def member_step(group):
        def step(member, carry):
            slot = group * held + member
            prepare(slot)
            compute(slot, member)

            @pl.when(jnp.logical_and(slot < early, lax.rem(slot, 2) == 1))
            def _():
                pair = pl.ds(slot - 1, 2)
                for_peers(lambda peer: copy(outgoing.at[peer, pair], incoming.at[me, pair], 0, peer).start())

            return carry

        return step

    lax.fori_loop(NARROW, held, member_step(0), 0)

    def group_step(group, carry):
        unpack(group + 1, range(held))
        lax.fori_loop(0, held, member_step(group), 0)
        return carry

    lax.fori_loop(1, slots // held, group_step, 0)

    pairs_group = 1 + chunks
    for_peers(lambda peer: copy(pair_row, pair_rows.at[me], pairs_group, peer).start())
    pair_rows[me] = pair_row[...]

    def chunk_step(index, carry):
        send_chunk(index)
        return carry

    lax.fori_loop(0, chunks, chunk_step, 0)

    others = pl.ds(0, devices - 1)
    whole = lambda ref: ref.at[others, pl.ds(0, early)]
    part = lambda ref, index: ref.at[others, pl.ds(early, slots - early), pl.ds(index * chunk, chunk), :]

    def wait_bytes(ref, sem):
        pltpu.make_async_copy(ref, ref, sem).wait()

    wait_bytes(pair_rows.at[others], recv_sem.at[pairs_group])

    def column_step(device, carry):
        row = pair_rows[device].astype(jnp.float32)
        rows = jnp.broadcast_to(row, (slots, row.shape[-1]))
        own = lax.broadcasted_iota(jnp.int32, rows.shape, 0) == lax.broadcasted_iota(jnp.int32, rows.shape, 1)
        column = jnp.sum(jnp.where(own, rows, 0.0), axis=1, keepdims=True)
        at = pl.ds(pl.multiple_of(device * slots, slots), slots)
        pair_columns[at, :] = jnp.broadcast_to(column, (slots, pair_columns.shape[1]))
        return carry

    lax.fori_loop(0, devices, column_step, 0)
    step = 64
    lane = lax.broadcasted_iota(jnp.int32, (step, total), 1)
    for low in range(0, total, step):
        pairs = pair_columns[low:low + step, :1].astype(jnp.int32)
        place[0, low:low + step, :] = (pairs == lane).astype(jnp.float32).astype(jnp.bfloat16)
        place[1, low:low + step, :] = (total - 1 - pairs == lane).astype(jnp.float32).astype(jnp.bfloat16)

    wait_bytes(whole(incoming), recv_sem.at[0])
    flat = recv.reshape(devices * slots * band, lanes)

    def place_step(index, carry):
        wait_bytes(part(incoming, index), recv_sem.at[1 + index])

        def store(i, w, values):
            row = index * chunk + i
            out_ref[row + side * (band - 1 - 2 * row), :, w * total:(w + 1) * total] = values

        place_rows(flat, place, high_rows, low_rows, index * chunk, chunk, band, store)
        return carry

    lax.fori_loop(0, chunks - 1, place_step, 0)
    wait_bytes(part(incoming, chunks - 1), recv_sem.at[chunks])

    wait_bytes(whole(outgoing), send_sem.at[0])

    def drain_step(index, carry):
        wait_bytes(part(outgoing, index), send_sem.at[1 + index])
        return carry

    lax.fori_loop(0, chunks, drain_step, 0)
    wait_bytes(pair_rows.at[others], send_sem.at[pairs_group])


def deliver_kernel(placed_ref, recv, place, out_ref, last, high_rows, low_rows, sems, *, devices):
    side = lax.div(lax.axis_index("ma"), devices // 2)
    band = out_ref.shape[0]
    count, _, total = last.shape
    total //= 2
    ready = pl.ds(side * count, band - count)
    bulk = pltpu.make_async_copy(placed_ref.at[ready], out_ref.at[ready], sems.at[0])
    bulk.start()
    flat = recv.reshape(total * band, recv.shape[-1])

    def store(i, w, values):
        to = i + side * (count - 1 - 2 * i)
        last[to, :, w * total:(w + 1) * total] = values

    place_rows(flat, place, high_rows, low_rows, band - count, count, band, store)
    tail = pltpu.make_async_copy(last, out_ref.at[pl.ds((1 - side) * (band - count), count)], sems.at[1])
    tail.start()
    bulk.wait()
    tail.wait()


def shards(coeffs, legendre, assign):
    devices = lax.axis_size("ma")
    slots, columns, width = coeffs.shape
    lat_half = legendre.shape[1]
    band = 2 * lat_half // devices
    total = devices * slots
    lanes = 2 * columns
    chunk = min(CHUNK_ROWS, band)
    early = max(slots // EARLY_PART // 2 * 2, NARROW)
    groups = 2 + band // chunk
    held = min(8, slots)
    main = width // SPAN * SPAN
    placed, received, place = pl.pallas_call(
        functools.partial(synthesis_kernel, devices=devices, early=early, chunk=chunk),
        out_shape=[
            pltpu.VMEM((band, columns, 2 * total), jnp.float32),
            pltpu.VMEM((devices, slots * band, lanes), jnp.float32),
            pltpu.VMEM((2, total, total), jnp.bfloat16),
        ],
        in_specs=[
            pl.BlockSpec(memory_space=pl.ANY),
            pl.BlockSpec(memory_space=pl.ANY),
            pl.BlockSpec(memory_space=pl.ANY),
        ],
        out_specs=[pl.BlockSpec(memory_space=pltpu.VMEM)] * 3,
        scratch_shapes=[
            pltpu.SMEM((slots,), jnp.int32),
            pltpu.VMEM((BUFFERS, columns, width), jnp.bfloat16),
            pltpu.VMEM((LOADS, SPAN, held, lat_half), jnp.bfloat16),
            pltpu.VMEM((width - main, slots, lat_half), jnp.bfloat16),
            pltpu.VMEM((width - main, slots, lat_half), jnp.float32),
            pltpu.VMEM((lat_half // 128, SPAN * held, 128), jnp.float32),
            pltpu.VMEM((held, main, lat_half), jnp.bfloat16),
            pltpu.VMEM((4 * columns, main), jnp.bfloat16),
            pltpu.VMEM((devices, slots * band, lanes), jnp.float32),
            pltpu.VMEM((1, lanes), jnp.int32),
            pltpu.VMEM((devices, 1, lanes), jnp.int32),
            pltpu.VMEM((total, lanes), jnp.float32),
            pltpu.VMEM((2, chunk * columns, total), jnp.bfloat16),
            pltpu.VMEM((2, chunk * columns, total), jnp.bfloat16),
            pltpu.SemaphoreType.DMA,
            pltpu.SemaphoreType.DMA((BUFFERS,)),
            pltpu.SemaphoreType.DMA((LOADS,)),
            pltpu.SemaphoreType.DMA,
            pltpu.SemaphoreType.DMA((groups,)),
            pltpu.SemaphoreType.DMA((groups,)),
        ],
        compiler_params=pltpu.CompilerParams(
            collective_id=0, has_side_effects=True, vmem_limit_bytes=40 * 1024 * 1024
        ),
        name="synthesis",
    )(assign, coeffs, legendre.transpose(2, 0, 1))
    return pl.pallas_call(
        functools.partial(deliver_kernel, devices=devices),
        out_shape=jax.ShapeDtypeStruct((band, columns, 2 * total), jnp.float32),
        in_specs=[pl.BlockSpec(memory_space=pltpu.VMEM)] * 3,
        out_specs=pl.BlockSpec(memory_space=pl.ANY),
        scratch_shapes=[
            pltpu.VMEM((chunk, columns, 2 * total), jnp.float32),
            pltpu.VMEM((2, chunk * columns, total), jnp.bfloat16),
            pltpu.VMEM((2, chunk * columns, total), jnp.bfloat16),
            pltpu.SemaphoreType.DMA((2,)),
        ],
        compiler_params=pltpu.CompilerParams(vmem_limit_bytes=8 * 1024 * 1024),
        name="deliver",
    )(placed, received, place)


def solution(mesh):
    return jax.shard_map(
        shards,
        mesh=mesh,
        in_specs=(P("ma", "af", None), P("ma", None, None), P("ma")),
        out_specs=P("ma", "af", None),
        check_vma=False,
    )
```
